128 devices in a mesh: data: 1, pp: 2 (over core), ep: 64 (over z, y, x).
Axes of the slice: x: 4, y: 4, z: 4, core: 2. Of those that a mesh axis runs over, the one named last changes fastest.
Arguments:
- expert_out: bfloat16 [2, 1, 128, 1024, 2048], P(('data', 'pp'), None, 'ep')
- expert_ids: int32 [2, 1, 64, 128, 8], P(('data', 'pp'), None, 'ep')
- slot_ids: int32 [2, 1, 64, 128, 8], P(('data', 'pp'), None, 'ep')
- gates: float32 [2, 1, 64, 128, 8], P(('data', 'pp'), None, 'ep')
- resid: bfloat16 [2, 1, 64, 128, 2048], P(('data', 'pp'), None, 'ep')
- norm_scale: float32 [2, 2048], P('pp')
- w_query: bfloat16 [2, 2048, 4096], P('pp')
- w_key: bfloat16 [2, 2048, 4096], P('pp')
- w_value: bfloat16 [2, 2048, 4096], P('pp')
- w_out: bfloat16 [2, 32, 128, 2048], P('pp')
Outputs:
- output: bfloat16 [2, 1, 64, 128, 2048], P(('data', 'pp'), None, 'ep')
All inputs are finite; a program needn't handle non-finite values.
Results may differ from the reference program's by a relative error of at most 0.00854844.
Values are sent between devices in bfloat16 or wider.
A program may use at most 1 GiB of HBM per device.

```python
import jax
import jax.numpy as jnp
from jax import lax

STAGES = 2
EP_DEVS = 64
MICRO = 1
SEQ_DEV = 1
SEQ_LEN = 128
MODEL_DIM = 2048
EXPERTS = 128
TOP_K = 8
HEADS = 32
HEAD_DIM = 128

TOK_DEV = SEQ_DEV * SEQ_LEN
TOKENS = TOK_DEV * EP_DEVS
SEQ_COUNT = SEQ_DEV * EP_DEVS
SLOT_DEV = 2 * TOK_DEV * TOP_K // EXPERTS
CAPACITY = SLOT_DEV * EP_DEVS
HOT_EXPERTS = EXPERTS // 4
HOT_PICKS = TOP_K // 2
HIDDEN = HEADS * HEAD_DIM
NORM_EPS = 1e-6
TOKEN_SHAPE = (STAGES, MICRO, SEQ_COUNT, SEQ_LEN)


def rank_in_group(group_ids):
    count = group_ids.shape[0]
    order = jnp.argsort(group_ids * count + jnp.arange(count))
    sorted_ids = group_ids[order]
    first_pos = jnp.searchsorted(sorted_ids, sorted_ids, side='left')
    sorted_rank = (jnp.arange(count) - first_pos).astype(jnp.int32)
    return jnp.zeros((count,), jnp.int32).at[order].set(sorted_rank)


def draw_group(group_key):
    perm_key, hot_key, cold_key = jax.random.split(group_key, 3)
    expert_order = jax.random.permutation(perm_key, EXPERTS)
    hot_list = expert_order[:HOT_EXPERTS]
    cold_list = expert_order[HOT_EXPERTS:]
    hot_score = jax.random.randint(hot_key, (TOKENS, HOT_EXPERTS), 0, 65536) * HOT_EXPERTS + jnp.arange(HOT_EXPERTS)
    cold_score = jax.random.randint(cold_key, (TOKENS, EXPERTS - HOT_EXPERTS), 0, 65536) * EXPERTS + jnp.arange(EXPERTS - HOT_EXPERTS)
    hot_pick = jnp.argsort(hot_score, axis=1)[:, :HOT_PICKS]
    cold_pick = jnp.argsort(cold_score, axis=1)[:, :TOP_K - HOT_PICKS]
    chosen = jnp.concatenate([hot_list[hot_pick], cold_list[cold_pick]], axis=1).astype(jnp.int32)
    ranks = jax.vmap(rank_in_group)(chosen.reshape(EP_DEVS, TOK_DEV * TOP_K))
    slot_base = (jnp.arange(EP_DEVS, dtype=jnp.int32) * SLOT_DEV)[:, None]
    slots = jnp.where(ranks < SLOT_DEV, ranks + slot_base, -1).astype(jnp.int32)
    return chosen, slots.reshape(TOKENS, TOP_K)


def draw_routing(route_key):
    group_keys = jax.random.split(route_key, STAGES * MICRO)
    chosen, slots = lax.map(draw_group, group_keys)
    full_shape = TOKEN_SHAPE + (TOP_K,)
    return chosen.reshape(full_shape), slots.reshape(full_shape)


def draw_stage_out(stage_key):
    scale_key, value_key = jax.random.split(stage_key)
    expert_scale = jnp.exp(0.5 * jax.random.normal(scale_key, (MICRO, EXPERTS, 1, 1), jnp.float32))
    raw_out = jax.random.normal(value_key, (MICRO, EXPERTS, CAPACITY, MODEL_DIM), jnp.float32)
    return (raw_out * expert_scale).astype(jnp.bfloat16)


def setup_inputs(seed: int = 0, part: int = 0) -> dict:
    part_key = jax.random.fold_in(jax.random.key(seed), part)
    route_key, gate_key, resid_key, out_key = jax.random.split(part_key, 4)
    shared = jax.random.split(jax.random.key(seed + 1), 5)
    expert_ids, slot_ids = draw_routing(route_key)
    gate_logits = 1.5 * jax.random.normal(gate_key, TOKEN_SHAPE + (TOP_K,), jnp.float32)
    gates = 2.0 * jax.nn.softmax(gate_logits, axis=-1)
    resid = jax.random.normal(resid_key, TOKEN_SHAPE + (MODEL_DIM,), jnp.float32).astype(jnp.bfloat16)
    expert_out = lax.map(draw_stage_out, jax.random.split(out_key, STAGES))
    norm_scale = 1.0 + 0.5 * jax.random.normal(shared[0], (STAGES, MODEL_DIM), jnp.float32)
    in_scale = MODEL_DIM ** -0.5
    w_query = (1.5 * in_scale * jax.random.normal(shared[1], (STAGES, MODEL_DIM, HIDDEN), jnp.float32)).astype(jnp.bfloat16)
    w_key = (in_scale * jax.random.normal(shared[2], (STAGES, MODEL_DIM, HIDDEN), jnp.float32)).astype(jnp.bfloat16)
    w_value = (in_scale * jax.random.normal(shared[3], (STAGES, MODEL_DIM, HIDDEN), jnp.float32)).astype(jnp.bfloat16)
    w_out = (2.0 * HIDDEN ** -0.5 * jax.random.normal(shared[4], (STAGES, HEADS, HEAD_DIM, MODEL_DIM), jnp.float32)).astype(jnp.bfloat16)
    return {'expert_out': expert_out, 'expert_ids': expert_ids, 'slot_ids': slot_ids, 'gates': gates, 'resid': resid, 'norm_scale': norm_scale, 'w_query': w_query, 'w_key': w_key, 'w_value': w_value, 'w_out': w_out}


def combine_group(group_args):
    row_table, flat_ids, weights, resid_rows = group_args
    running = resid_rows.astype(jnp.float32)
    for choice in range(TOP_K):
        running = running + weights[:, choice, None] * row_table[flat_ids[:, choice]].astype(jnp.float32)
    return running.astype(jnp.bfloat16)


def attend_sequence(seq_rows, gain_row, w_query, w_key, w_value, w_out):
    x_float = seq_rows.astype(jnp.float32)
    inv_rms = lax.rsqrt(jnp.mean(x_float * x_float, axis=-1, keepdims=True) + NORM_EPS)
    normed = (x_float * inv_rms * gain_row).astype(jnp.bfloat16)
    q_heads = jnp.dot(normed, w_query, preferred_element_type=jnp.float32).astype(jnp.bfloat16).reshape(SEQ_LEN, HEADS, HEAD_DIM)
    k_heads = jnp.dot(normed, w_key, preferred_element_type=jnp.float32).astype(jnp.bfloat16).reshape(SEQ_LEN, HEADS, HEAD_DIM)
    v_heads = jnp.dot(normed, w_value, preferred_element_type=jnp.float32).astype(jnp.bfloat16).reshape(SEQ_LEN, HEADS, HEAD_DIM)
    scores = jnp.einsum('qhe,khe->hqk', q_heads.astype(jnp.float32), k_heads.astype(jnp.float32)) * HEAD_DIM ** -0.5
    positions = jnp.arange(SEQ_LEN)
    causal = positions[:, None] >= positions[None, :]
    attn_prob = jax.nn.softmax(jnp.where(causal, scores, -jnp.inf), axis=-1).astype(jnp.bfloat16)
    context = jnp.einsum('hqk,khe->qhe', attn_prob.astype(jnp.float32), v_heads.astype(jnp.float32)).astype(jnp.bfloat16)
    proj = jnp.einsum('qhe,hed->qd', context.astype(jnp.float32), w_out.astype(jnp.float32)).astype(jnp.bfloat16)
    return (x_float + proj.astype(jnp.float32)).astype(jnp.bfloat16)


def reference(expert_out, expert_ids, slot_ids, gates, resid, norm_scale, w_query, w_key, w_value, w_out):
    groups = STAGES * MICRO
    row_table = expert_out.reshape(groups, EXPERTS * CAPACITY, MODEL_DIM)
    is_kept = slot_ids >= 0
    flat_ids = (expert_ids * CAPACITY + jnp.where(is_kept, slot_ids, 0)).reshape(groups, TOKENS, TOP_K)
    weights = jnp.where(is_kept, gates, 0.0).reshape(groups, TOKENS, TOP_K)
    resid_rows = resid.reshape(groups, TOKENS, MODEL_DIM)
    combined = lax.map(combine_group, (row_table, flat_ids, weights, resid_rows))
    shifted = jnp.roll(combined.reshape(STAGES, MICRO * SEQ_COUNT, SEQ_LEN, MODEL_DIM), 1, axis=0)

    def stage_block(stage_args):
        stage_seqs, gain_row, stage_query, stage_key, stage_value, stage_out = stage_args

        def one_sequence(seq_rows):
            return attend_sequence(seq_rows, gain_row, stage_query, stage_key, stage_value, stage_out)

        return lax.map(one_sequence, stage_seqs)

    result = lax.map(stage_block, (shifted, norm_scale, w_query, w_key, w_value, w_out))
    return result.reshape(TOKEN_SHAPE + (MODEL_DIM,))
```

```python
import functools
import jax
import jax.numpy as jnp
from jax import lax
from jax.experimental import pallas as pl
from jax.experimental.pallas import tpu as pltpu
from jax.sharding import PartitionSpec as P

NORM_EPS = 1e-6
MESH = pl.DeviceIdType.MESH
STRIDES = (1, 4, 16)
BF16_MAX = 3.3895313892515355e38


def axis_coord(me, dim):
    return lax.rem(lax.div(me, STRIDES[dim]), 4)


def mate_of(me, dim, hop):
    coord = axis_coord(me, dim)
    return me + (lax.rem(coord + hop, 4) - coord) * STRIDES[dim]


def exchange_kernel(bounds, eo, meta, resid, y_ref, p1, p2, s3, r3, metas, gates, res_buf,
                    p1s, p1r, p2s, p2r, p3s, p3r, ms, mr, rs, rr):
    me = lax.axis_index('ep')
    pp = lax.axis_index('pp')
    other = 1 - pp
    coords = tuple(axis_coord(me, dim) for dim in range(3))

    barrier = pltpu.get_barrier_semaphore()
    for dim in range(3):
        for hop in range(1, 4):
            for stage in (pp, other):
                pl.semaphore_signal(barrier, inc=1, device_id={'pp': stage, 'ep': mate_of(me, dim, hop)}, device_id_type=MESH)
    pl.semaphore_signal(barrier, inc=1, device_id={'pp': other, 'ep': me}, device_id_type=MESH)
    pl.semaphore_wait(barrier, 19)

    def meta_copy(dim, hop):
        return pltpu.make_async_remote_copy(meta, metas.at[dim, hop], ms.at[dim, hop], mr.at[dim, hop],
                                            device_id={'pp': pp, 'ep': mate_of(me, dim, 4 - hop)}, device_id_type=MESH)

    for dim in range(3):
        for hop in range(1, 4):
            meta_copy(dim, hop).start()
    resid_copy = pltpu.make_async_remote_copy(resid, res_buf, rs, rr, device_id={'pp': other, 'ep': me}, device_id_type=MESH)
    resid_copy.start()

    def columns(tile):
        return pl.ds(pl.multiple_of(tile * 128, 128), 128)

    def rows_for(dim, coord, tile):
        if dim == 0:
            return eo.at[:, :, :, coord, :, columns(tile)]
        if dim == 1:
            return eo.at[:, :, coord, :, :, columns(tile)]
        return eo.at[:, coord, :, :, :, columns(tile)]

    def first_copy(c, tile, hop):
        return pltpu.make_async_remote_copy(rows_for(c, lax.rem(coords[c] + hop, 4), tile), p1.at[tile, hop],
                                            p1s.at[tile, hop], p1r.at[tile, hop],
                                            device_id={'pp': pp, 'ep': mate_of(me, c, hop)}, device_id_type=MESH)

    def own_copy(c, tile):
        return pltpu.make_async_copy(rows_for(c, coords[c], tile), p1.at[tile, 0], p1r.at[tile, 0])

    def second_copy(c, tile, hop):
        dim = (c + 1) % 3
        coord = lax.rem(coords[dim] + hop, 4)
        src = p1.at[tile, :, :, coord] if c == 1 else p1.at[tile, :, :, :, coord]
        return pltpu.make_async_remote_copy(src, p2.at[tile, hop - 1], p2s.at[tile, hop - 1], p2r.at[tile, hop - 1],
                                            device_id={'pp': pp, 'ep': mate_of(me, dim, hop)}, device_id_type=MESH)

    def third_copy(c, tile, hop):
        dim = (c + 2) % 3
        return pltpu.make_async_remote_copy(s3.at[tile, hop], r3.at[hop, :, columns(tile)], p3s.at[tile, hop], p3r.at[tile, hop],
                                            device_id={'pp': other, 'ep': mate_of(me, dim, hop)}, device_id_type=MESH)

    def for_tiles(body):
        short = min(bounds[c + 1] - bounds[c] for c in range(3))

        @pl.loop(0, short)
        def _(step):
            for c in range(3):
                body(c, bounds[c] + step)
        for c in range(3):
            for tile in range(bounds[c] + short, bounds[c + 1]):
                body(c, tile)

    def start_first(c, tile):
        for hop in range(1, 4):
            first_copy(c, tile, hop).start()
        own_copy(c, tile).start()

    for_tiles(start_first)

    metas[0, 0] = meta[...]
    metas[1, 0] = meta[...]
    metas[2, 0] = meta[...]
    for dim in range(3):
        for hop in range(1, 4):
            meta_copy(dim, hop).wait_recv()
    lane = lax.broadcasted_iota(jnp.int32, (1, 128), 1)
    for c in range(3):
        d1, d2, d3 = c, (c + 1) % 3, (c + 2) % 3
        hop1 = (lane // 32) % 4
        local = lane % 32
        first = ((coords[d1] - hop1 + 4) % 4) * STRIDES[d1] + coords[d3] * STRIDES[d3]

        @pl.loop(0, 4)
        def _(w):
            table = jnp.transpose(metas[d3, w])
            for hop2 in range(4):
                src = first + lax.rem(coords[d2] - hop2 + 4, 4) * STRIDES[d2]
                row_id = (src * 32 + local).astype(jnp.float32)
                gate = jnp.zeros((128, 128), jnp.float32)
                for j in range(8):
                    gate = jnp.where(table[:, j:j + 1] == row_id, table[:, 8 + j:9 + j], gate)
                high = jnp.minimum(gate, BF16_MAX).astype(jnp.bfloat16)
                rest = gate - high.astype(jnp.float32)
                mid = rest.astype(jnp.bfloat16)
                low = (rest - mid.astype(jnp.float32)).astype(jnp.bfloat16)
                gates[c, w, 0:128, hop2 * 128:hop2 * 128 + 128] = high
                gates[c, w, 128:256, hop2 * 128:hop2 * 128 + 128] = mid
                gates[c, w, 256:384, hop2 * 128:hop2 * 128 + 128] = low

    def relay(c, tile):
        own_copy(c, tile).wait()
        for hop in range(1, 4):
            first_copy(c, tile, hop).wait_recv()
        for hop in range(1, 4):
            second_copy(c, tile, hop).start()

    for_tiles(relay)

    def partial_sums(c, tile):
        dim2, dim3 = (c + 1) % 3, (c + 2) % 3
        for hop in range(1, 4):
            second_copy(c, tile, hop).wait_recv()

        @pl.loop(0, 4)
        def _(w):
            coord = lax.rem(coords[dim3] + w, 4)
            own = coords[dim2]
            if c == 1:
                blocks = [p1[tile, :, :, own, coord]]
            else:
                blocks = [p1[tile, :, :, coord, own]]
            blocks += [p2[tile, hop, :, :, coord] for hop in range(3)]
            rows = jnp.concatenate([b.reshape(128, 128) for b in blocks], axis=0)
            parts = jnp.dot(gates[c, w], rows, preferred_element_type=jnp.float32)
            s3[tile, w] = parts[0:128] + parts[128:256] + parts[256:384]
            third_copy(c, tile, w).start()

    for_tiles(partial_sums)

    resid_copy.wait_recv()

    def finish(c, tile):
        for hop in range(4):
            third_copy(c, tile, hop).wait_recv()
        cols = columns(tile)
        total = res_buf[:, cols].astype(jnp.float32)
        for hop in range(4):
            total = total + r3[hop, :, cols]
        y_ref[:, cols] = total.astype(jnp.bfloat16)

    for_tiles(finish)

    def drain(c, tile):
        for hop in range(1, 4):
            first_copy(c, tile, hop).wait_send()
            second_copy(c, tile, hop).wait_send()
        for hop in range(4):
            third_copy(c, tile, hop).wait_send()

    for_tiles(drain)
    for dim in range(3):
        for hop in range(1, 4):
            meta_copy(dim, hop).wait_send()
    resid_copy.wait_send()


def exchange(eo, meta, resid):
    tiles = eo.shape[-1] // 128
    bounds = (0, tiles // 3, 2 * (tiles // 3), tiles)
    dma = pltpu.SemaphoreType.DMA
    return pl.pallas_call(
        functools.partial(exchange_kernel, bounds),
        out_shape=jax.ShapeDtypeStruct(resid.shape, jnp.bfloat16),
        in_specs=[pl.BlockSpec(memory_space=pl.ANY), pl.BlockSpec(memory_space=pltpu.VMEM), pl.BlockSpec(memory_space=pl.ANY)],
        out_specs=pl.BlockSpec(memory_space=pltpu.VMEM),
        scratch_shapes=[
            pltpu.VMEM((tiles, 4, 2, 4, 4, 16, 128), jnp.bfloat16),
            pltpu.VMEM((tiles, 3, 4, 2, 4, 16, 128), jnp.bfloat16),
            pltpu.VMEM((tiles, 4, 128, 128), jnp.float32),
            pltpu.VMEM((4, 128, tiles * 128), jnp.float32),
            pltpu.VMEM((3, 4, 16, 128), jnp.float32),
            pltpu.VMEM((3, 4, 384, 512), jnp.bfloat16),
            pltpu.VMEM(resid.shape, jnp.bfloat16),
            dma((tiles, 4)), dma((tiles, 4)), dma((tiles, 3)), dma((tiles, 3)), dma((tiles, 4)), dma((tiles, 4)),
            dma((3, 4)), dma((3, 4)), dma, dma,
        ],
        compiler_params=pltpu.CompilerParams(collective_id=0, has_side_effects=True, vmem_limit_bytes=60 * 2**20),
    )(eo, meta, resid)


def attend_block(arrived, gain_row, w_query, w_key, w_value, w_out):
    head_count, head_dim = w_out.shape[0], w_out.shape[1]
    seq_len = arrived.shape[0]
    x_float = arrived.astype(jnp.float32)
    inv_rms = lax.rsqrt(jnp.mean(jnp.square(x_float), axis=-1, keepdims=True) + NORM_EPS)
    normed = (x_float * inv_rms * gain_row).astype(jnp.bfloat16)

    def project(w_mat):
        return jnp.dot(normed, w_mat, preferred_element_type=jnp.float32).astype(jnp.bfloat16).reshape(seq_len, head_count, head_dim)

    q_heads = project(w_query)
    k_heads = project(w_key)
    v_heads = project(w_value)
    scores = jnp.einsum('qhe,khe->hqk', q_heads, k_heads, preferred_element_type=jnp.float32) * head_dim ** -0.5
    positions = jnp.arange(seq_len)
    causal = positions[:, None] >= positions[None, :]
    attn_prob = jax.nn.softmax(jnp.where(causal, scores, -jnp.inf), axis=-1).astype(jnp.bfloat16)
    context = jnp.einsum('hqk,khe->qhe', attn_prob, v_heads, preferred_element_type=jnp.float32).astype(jnp.bfloat16)
    proj = jnp.einsum('qhe,hed->qd', context, w_out, preferred_element_type=jnp.float32).astype(jnp.bfloat16)
    return (x_float + proj.astype(jnp.float32)).astype(jnp.bfloat16)


def solution(mesh):
    token_spec = P(('data', 'pp'), None, 'ep', None, None)
    weight_spec = P('pp', None, None)

    def local_step(expert_out, expert_ids, slot_ids, gates, resid, norm_scale, w_query, w_key, w_value, w_out):
        eo = expert_out.reshape(2, 4, 4, 4, 16, expert_out.shape[-1])
        slots = slot_ids[0, 0, 0]
        kept = slots >= 0
        local = slots - lax.axis_index('ep') * 16
        flat = jnp.where(kept, expert_ids[0, 0, 0] * 16 + local, -1).astype(jnp.float32)
        weights = jnp.where(kept, gates[0, 0, 0], 0.0)
        meta = jnp.concatenate([flat.T, weights.T], axis=0)
        arrived = exchange(eo, meta, resid[0, 0, 0])
        result = attend_block(arrived, norm_scale[0], w_query[0], w_key[0], w_value[0], w_out[0])
        return result[None, None, None]

    return jax.shard_map(local_step, mesh=mesh, in_specs=(token_spec, token_spec, token_spec, token_spec, token_spec, P('pp', None), weight_spec, weight_spec, weight_spec, P('pp', None, None, None)), out_specs=token_spec, check_vma=False)
```

```python
import functools
import jax
import jax.numpy as jnp
from jax import lax
from jax.experimental import pallas as pl
from jax.experimental.pallas import tpu as pltpu
from jax.sharding import PartitionSpec as P

NORM_EPS = 1e-6
MESH = pl.DeviceIdType.MESH
STRIDES = (1, 4, 16)
BF16_MAX = 3.3895313892515355e38
GROUP = 512
GROUPS = 8
PIECES = 32
RING = 15


def axis_coord(me, dim):
    return lax.rem(lax.div(me, STRIDES[dim]), 4)


def mate_of(me, dim, hop):
    coord = axis_coord(me, dim)
    return me + (lax.rem(coord + hop, 4) - coord) * STRIDES[dim]


def stage_kernel(bounds, eo, ids, slots, gate_in, resid, gain, wq, wk, wv, wo, out_ref, p1, p2, s3, r3, ids_all, slots_all,
                 gates_all, gates, res_buf, y_ref, x_ref, qkv, context, slab, p1s, p1r, p2s, p2r, p3s, p3r, ms, mr, rs, rr, wsem):
    me = lax.axis_index('ep')
    pp = lax.axis_index('pp')
    other = 1 - pp
    coords = tuple(axis_coord(me, dim) for dim in range(3))

    barrier = pltpu.get_barrier_semaphore()
    for dim in range(3):
        for hop in range(1, 4):
            for stage in (pp, other):
                pl.semaphore_signal(barrier, inc=1, device_id={'pp': stage, 'ep': mate_of(me, dim, hop)}, device_id_type=MESH)
    pl.semaphore_signal(barrier, inc=1, device_id={'pp': other, 'ep': me}, device_id_type=MESH)
    pl.semaphore_wait(barrier, 19)

    routing = ((ids, ids_all), (slots, slots_all), (gate_in, gates_all))

    def meta_copies(dim, hop):
        return [pltpu.make_async_remote_copy(src, dst.at[dim, hop], ms.at[i, dim, hop], mr.at[i, dim, hop],
                                             device_id={'pp': pp, 'ep': mate_of(me, dim, 4 - hop)}, device_id_type=MESH)
                for i, (src, dst) in enumerate(routing)]

    for dim in range(3):
        for hop in range(1, 4):
            for copy in meta_copies(dim, hop):
                copy.start()
    resid_copy = pltpu.make_async_remote_copy(resid, res_buf, rs, rr, device_id={'pp': other, 'ep': me}, device_id_type=MESH)
    resid_copy.start()

    def columns(tile):
        return pl.ds(pl.multiple_of(tile * 128, 128), 128)

    def rows_for(dim, coord, tile):
        if dim == 0:
            return eo.at[:, :, :, coord, :, columns(tile)]
        if dim == 1:
            return eo.at[:, :, coord, :, :, columns(tile)]
        return eo.at[:, coord, :, :, :, columns(tile)]

    def first_copy(c, tile, hop):
        return pltpu.make_async_remote_copy(rows_for(c, lax.rem(coords[c] + hop, 4), tile), p1.at[tile, hop],
                                            p1s.at[tile, hop], p1r.at[tile, hop],
                                            device_id={'pp': pp, 'ep': mate_of(me, c, hop)}, device_id_type=MESH)

    def own_copy(c, tile):
        return pltpu.make_async_copy(rows_for(c, coords[c], tile), p1.at[tile, 0], p1r.at[tile, 0])

    def second_copy(c, tile, hop):
        dim = (c + 1) % 3
        coord = lax.rem(coords[dim] + hop, 4)
        src = p1.at[tile, :, :, coord] if c == 1 else p1.at[tile, :, :, :, coord]
        return pltpu.make_async_remote_copy(src, p2.at[tile, hop - 1], p2s.at[tile, hop - 1], p2r.at[tile, hop - 1],
                                            device_id={'pp': pp, 'ep': mate_of(me, dim, hop)}, device_id_type=MESH)

    def third_copy(c, tile, hop):
        dim = (c + 2) % 3
        return pltpu.make_async_remote_copy(s3.at[tile, hop], r3.at[hop, :, columns(tile)], p3s.at[tile, hop], p3r.at[tile, hop],
                                            device_id={'pp': other, 'ep': mate_of(me, dim, hop)}, device_id_type=MESH)

    def third_wait(tile, hop):
        third_copy(0, tile, hop).wait_recv()

    def slab_wait(slot):
        pltpu.make_async_copy(wq.at[:, pl.ds(0, GROUP)], slab.at[slot], wsem.at[slot]).wait()

    def qkv_load(group, i):
        slot = lax.rem(group, RING // 3) * 3 + i
        return pltpu.make_async_copy((wq, wk, wv)[i].at[:, pl.ds(pl.multiple_of(group * GROUP, GROUP), GROUP)], slab.at[slot], wsem.at[slot])

    def out_load(piece):
        chunk, half = (piece - GROUPS * 3) // 2, piece % 2
        return pltpu.make_async_copy(wo.at[pl.ds(half * 2048, 2048), pl.ds(chunk * GROUP, GROUP)], slab.at[piece % RING], wsem.at[piece % RING])

    def for_tiles(body):
        short = min(bounds[c + 1] - bounds[c] for c in range(3))

        @pl.loop(0, short)
        def _(step):
            for c in range(3):
                body(c, bounds[c] + step)
        for c in range(3):
            for tile in range(bounds[c] + short, bounds[c + 1]):
                body(c, tile)

    def start_first(c, tile):
        for hop in range(1, 4):
            first_copy(c, tile, hop).start()
        own_copy(c, tile).start()

    for_tiles(start_first)

    for dim in range(3):
        for src, dst in routing:
            dst[dim, 0] = src[...]
        for hop in range(1, 4):
            for copy in meta_copies(dim, hop):
                copy.wait_recv()
    lane = lax.broadcasted_iota(jnp.int32, (1, 128), 1)
    for c in range(3):
        d1, d2, d3 = c, (c + 1) % 3, (c + 2) % 3
        hop1 = (lane // 32) % 4
        local = lane % 32
        first = ((coords[d1] - hop1 + 4) % 4) * STRIDES[d1] + coords[d3] * STRIDES[d3]

        @pl.loop(0, 4)
        def _(w):
            owner = coords[d1] * STRIDES[d1] + coords[d2] * STRIDES[d2] + lax.rem(coords[d3] + w, 4) * STRIDES[d3]
            slot = slots_all[d3, w]
            flat = jnp.where(slot >= 0, ids_all[d3, w] * 16 + slot - owner * 16, -1)
            table = jnp.transpose(jnp.concatenate([flat.astype(jnp.float32), gates_all[d3, w]], axis=0))
            for hop2 in range(4):
                src = first + lax.rem(coords[d2] - hop2 + 4, 4) * STRIDES[d2]
                row_id = (src * 32 + local).astype(jnp.float32)
                gate = jnp.zeros((128, 128), jnp.float32)
                for j in range(8):
                    gate = jnp.where(table[:, j:j + 1] == row_id, table[:, 8 + j:9 + j], gate)
                high = jnp.minimum(gate, BF16_MAX).astype(jnp.bfloat16)
                rest = gate - high.astype(jnp.float32)
                mid = rest.astype(jnp.bfloat16)
                low = (rest - mid.astype(jnp.float32)).astype(jnp.bfloat16)
                gates[c, w, 0:128, hop2 * 128:hop2 * 128 + 128] = high
                gates[c, w, 128:256, hop2 * 128:hop2 * 128 + 128] = mid
                gates[c, w, 256:384, hop2 * 128:hop2 * 128 + 128] = low

    def relay(c, tile):
        own_copy(c, tile).wait()
        for hop in range(1, 4):
            first_copy(c, tile, hop).wait_recv()
        for hop in range(1, 4):
            second_copy(c, tile, hop).start()

    for_tiles(relay)

    for group in range(RING // 3):
        for i in range(3):
            qkv_load(group, i).start()

    def partial_sums(c, tile):
        dim2, dim3 = (c + 1) % 3, (c + 2) % 3
        for hop in range(1, 4):
            second_copy(c, tile, hop).wait_recv()

        @pl.loop(0, 4)
        def _(w):
            coord = lax.rem(coords[dim3] + w, 4)
            own = coords[dim2]
            if c == 1:
                blocks = [p1[tile, :, :, own, coord]]
            else:
                blocks = [p1[tile, :, :, coord, own]]
            blocks += [p2[tile, hop, :, :, coord] for hop in range(3)]
            rows = jnp.concatenate([b.reshape(128, 128) for b in blocks], axis=0)
            parts = jnp.dot(gates[c, w], rows, preferred_element_type=jnp.float32)
            s3[tile, w] = parts[0:128] + parts[128:256] + parts[256:384]
            third_copy(c, tile, w).start()

    for_tiles(partial_sums)

    resid_copy.wait_recv()

    @pl.loop(0, 4)
    def _(part):
        cols = pl.ds(pl.multiple_of(part * 512, 512), 512)

        @pl.loop(0, 4)
        def _(quarter):
            for hop in range(4):
                third_wait(part * 4 + quarter, hop)
        total = res_buf[:, cols].astype(jnp.float32)
        for hop in range(4):
            total = total + r3[hop, :, cols]
        y_ref[:, cols] = total.astype(jnp.bfloat16)

    y_float = y_ref[...].astype(jnp.float32)
    scale = lax.rsqrt(jnp.sum(y_float * y_float, axis=-1, keepdims=True) * (1.0 / y_ref.shape[1]) + NORM_EPS)
    x_ref[...] = (y_float * scale * gain[...]).astype(jnp.bfloat16)

    def attend(group):
        rows = lax.broadcasted_iota(jnp.int32, (128, 128), 0)
        keys = lax.broadcasted_iota(jnp.int32, (128, 128), 1)
        outs = []
        for head in range(GROUP // 128):
            lanes = slice(head * 128, head * 128 + 128)
            score = lax.dot_general(qkv[0, :, lanes], qkv[1, :, lanes], (((1,), (1,)), ((), ())), preferred_element_type=jnp.float32)
            score = jnp.where(rows >= keys, score * 128 ** -0.5, -jnp.inf)
            weight = jnp.exp(score - jnp.max(score, axis=-1, keepdims=True))
            prob = (weight / jnp.sum(weight, axis=-1, keepdims=True)).astype(jnp.bfloat16)
            outs.append(jnp.dot(prob, qkv[2, :, lanes], preferred_element_type=jnp.float32).astype(jnp.bfloat16))
        context[:, pl.ds(pl.multiple_of(group * GROUP, GROUP), GROUP)] = jnp.concatenate(outs, axis=1)

    @pl.loop(0, GROUPS)
    def _(group):
        base = lax.rem(group, RING // 3) * 3
        for i in range(3):
            slab_wait(base + i)
        fresh = [jnp.dot(x_ref[...], slab[base + i], preferred_element_type=jnp.float32).astype(jnp.bfloat16) for i in range(3)]

        @pl.when(group > 0)
        def _():
            attend(group - 1)
        for i in range(3):
            qkv[i] = fresh[i]

        @pl.when(group + RING // 3 < GROUPS)
        def _():
            for i in range(3):
                qkv_load(group + RING // 3, i).start()
        for late in range(GROUPS - RING // 3, GROUPS):
            if (late + RING // 3) * 3 < PIECES:
                @pl.when(group == late)
                def _():
                    for piece in range((late + RING // 3) * 3, min((late + RING // 3) * 3 + 3, PIECES)):
                        out_load(piece).start()

    attend(GROUPS - 1)

    for chunk in range(PIECES // 2 - GROUPS * 3 // 2):
        total = jnp.zeros((128, GROUP), jnp.float32)
        for half in range(2):
            piece = GROUPS * 3 + chunk * 2 + half
            slab_wait(piece % RING)
            total = total + jnp.dot(context[:, half * 2048:half * 2048 + 2048], slab[piece % RING], preferred_element_type=jnp.float32)
        cols = slice(chunk * GROUP, chunk * GROUP + GROUP)
        out_ref[:, cols] = (y_ref[:, cols].astype(jnp.float32) + total.astype(jnp.bfloat16).astype(jnp.float32)).astype(jnp.bfloat16)

    def drain(c, tile):
        for hop in range(1, 4):
            first_copy(c, tile, hop).wait_send()
            second_copy(c, tile, hop).wait_send()
        for hop in range(4):
            third_copy(c, tile, hop).wait_send()

    for_tiles(drain)
    for dim in range(3):
        for hop in range(1, 4):
            for copy in meta_copies(dim, hop):
                copy.wait_send()
    resid_copy.wait_send()


def run_stage(eo, ids, slots, gate_in, resid, gain, wq, wk, wv, wo):
    tiles = eo.shape[-1] // 128
    bounds = (0, tiles // 3, 2 * (tiles // 3), tiles)
    dma = pltpu.SemaphoreType.DMA
    hbm = pl.BlockSpec(memory_space=pl.ANY)
    vmem = pl.BlockSpec(memory_space=pltpu.VMEM)
    return pl.pallas_call(
        functools.partial(stage_kernel, bounds),
        out_shape=jax.ShapeDtypeStruct(resid.shape, jnp.bfloat16),
        in_specs=[hbm, vmem, vmem, vmem, hbm, vmem, hbm, hbm, hbm, hbm],
        out_specs=vmem,
        scratch_shapes=[
            pltpu.VMEM((tiles, 4, 2, 4, 4, 16, 128), jnp.bfloat16),
            pltpu.VMEM((tiles, 3, 4, 2, 4, 16, 128), jnp.bfloat16),
            pltpu.VMEM((tiles, 4, 128, 128), jnp.float32),
            pltpu.VMEM((4, 128, tiles * 128), jnp.float32),
            pltpu.VMEM((3, 4, 8, 128), jnp.int32),
            pltpu.VMEM((3, 4, 8, 128), jnp.int32),
            pltpu.VMEM((3, 4, 8, 128), jnp.float32),
            pltpu.VMEM((3, 4, 384, 512), jnp.bfloat16),
            pltpu.VMEM(resid.shape, jnp.bfloat16),
            pltpu.VMEM(resid.shape, jnp.bfloat16),
            pltpu.VMEM(resid.shape, jnp.bfloat16),
            pltpu.VMEM((3, 128, GROUP), jnp.bfloat16),
            pltpu.VMEM((128, wq.shape[1]), jnp.bfloat16),
            pltpu.VMEM((RING, 2048, GROUP), jnp.bfloat16),
            dma((tiles, 4)), dma((tiles, 4)), dma((tiles, 3)), dma((tiles, 3)), dma((tiles, 4)), dma((tiles, 4)),
            dma((3, 3, 4)), dma((3, 3, 4)), dma, dma, dma((RING,)),
        ],
        compiler_params=pltpu.CompilerParams(collective_id=0, has_side_effects=True, vmem_limit_bytes=67043328),
    )(eo, ids, slots, gate_in, resid, gain, wq, wk, wv, wo)


def solution(mesh):
    token_spec = P(('data', 'pp'), None, 'ep', None, None)
    weight_spec = P('pp', None, None)

    def local_step(expert_out, expert_ids, slot_ids, gates, resid, norm_scale, w_query, w_key, w_value, w_out):
        eo = expert_out.reshape(2, 4, 4, 4, 16, expert_out.shape[-1])
        result = run_stage(eo, expert_ids[0, 0, 0].T, slot_ids[0, 0, 0].T, gates[0, 0, 0].T, resid[0, 0, 0], norm_scale,
                           w_query[0], w_key[0], w_value[0], w_out[0].reshape(-1, w_out.shape[-1]))
        return result[None, None, None]

    return jax.shard_map(local_step, mesh=mesh, in_specs=(token_spec, token_spec, token_spec, token_spec, token_spec, P('pp', None), weight_spec, weight_spec, weight_spec, P('pp', None, None, None)), out_specs=token_spec, check_vma=False)
```

```python
import functools
import jax
import jax.numpy as jnp
from jax import lax
from jax.experimental import pallas as pl
from jax.experimental.pallas import tpu as pltpu
from jax.sharding import PartitionSpec as P

NORM_EPS = 1e-6
MESH = pl.DeviceIdType.MESH
STRIDES = (1, 4, 16)
BF16_MAX = 3.3895313892515355e38
GROUP = 512
GROUPS = 8
CHUNKS = 4
RING = 15


def axis_coord(me, dim):
    return lax.rem(lax.div(me, STRIDES[dim]), 4)


def mate_of(me, dim, hop):
    coord = axis_coord(me, dim)
    return me + (lax.rem(coord + hop, 4) - coord) * STRIDES[dim]


def stage_kernel(bounds, eo, ids, slots, gate_in, resid, gain, wq, wk, wv, wo, wo_flat, out_ref, p1, p2, s3, r3, ids_all, slots_all,
                 gates_all, gates, res_buf, y_ref, x_ref, qkv, context, slab, p1s, p1r, p2s, p2r, p3s, p3r, ms, mr, rs, rr, wsem, hsem, keys_t):
    me = lax.axis_index('ep')
    pp = lax.axis_index('pp')
    other = 1 - pp
    coords = tuple(axis_coord(me, dim) for dim in range(3))

    barrier = pltpu.get_barrier_semaphore()
    for dim in range(3):
        for hop in range(1, 4):
            for stage in (pp, other):
                pl.semaphore_signal(barrier, inc=1, device_id={'pp': stage, 'ep': mate_of(me, dim, hop)}, device_id_type=MESH)
    pl.semaphore_signal(barrier, inc=1, device_id={'pp': other, 'ep': me}, device_id_type=MESH)
    pl.semaphore_wait(barrier, 19)

    routing = ((ids, ids_all), (slots, slots_all), (gate_in, gates_all))

    def meta_copies(dim, hop):
        return [pltpu.make_async_remote_copy(src, dst.at[dim, hop], ms.at[i, dim, hop], mr.at[i, dim, hop],
                                             device_id={'pp': pp, 'ep': mate_of(me, dim, 4 - hop)}, device_id_type=MESH)
                for i, (src, dst) in enumerate(routing)]

    for dim in range(3):
        for hop in range(1, 4):
            for copy in meta_copies(dim, hop):
                copy.start()
    for dim in range(3):
        for i, (src, dst) in enumerate(routing):
            pltpu.make_async_copy(src, dst.at[dim, 0], ms.at[i, dim, 0]).start()
    resid_copy = pltpu.make_async_remote_copy(resid, res_buf, rs, rr, device_id={'pp': other, 'ep': me}, device_id_type=MESH)
    resid_copy.start()

    def columns(tile):
        return pl.ds(pl.multiple_of(tile * 128, 128), 128)

    def rows_for(dim, coord, tile):
        if dim == 0:
            return eo.at[:, :, :, coord, :, columns(tile)]
        if dim == 1:
            return eo.at[:, :, coord, :, :, columns(tile)]
        return eo.at[:, coord, :, :, :, columns(tile)]

    def first_copy(c, tile, hop):
        return pltpu.make_async_remote_copy(rows_for(c, lax.rem(coords[c] + hop, 4), tile), p1.at[tile, hop],
                                            p1s.at[tile, hop], p1r.at[tile, hop],
                                            device_id={'pp': pp, 'ep': mate_of(me, c, hop)}, device_id_type=MESH)

    def own_copy(c, tile):
        return pltpu.make_async_copy(rows_for(c, coords[c], tile), p1.at[tile, 0], p1r.at[tile, 0])

    def second_copy(c, tile, hop):
        dim = (c + 1) % 3
        coord = lax.rem(coords[dim] + hop, 4)
        src = p1.at[tile, :, :, coord] if c == 1 else p1.at[tile, :, :, :, coord]
        return pltpu.make_async_remote_copy(src, p2.at[tile, hop - 1], p2s.at[tile, hop - 1], p2r.at[tile, hop - 1],
                                            device_id={'pp': pp, 'ep': mate_of(me, dim, hop)}, device_id_type=MESH)

    def third_copy(c, tile, hop):
        dim = (c + 2) % 3
        return pltpu.make_async_remote_copy(s3.at[tile, hop], r3.at[hop, :, columns(tile)], p3s.at[tile, hop], p3r.at[tile, hop],
                                            device_id={'pp': other, 'ep': mate_of(me, dim, hop)}, device_id_type=MESH)

    def third_wait(tile, hop):
        third_copy(0, tile, hop).wait_recv()

    def slab_wait(slot):
        pltpu.make_async_copy(wq.at[:, pl.ds(0, GROUP)], slab.at[slot], wsem.at[slot]).wait()

    def qkv_load(group, i):
        slot = lax.rem(group, RING // 3) * 3 + i
        return pltpu.make_async_copy((wq, wk, wv)[i].at[:, pl.ds(pl.multiple_of(group * GROUP, GROUP), GROUP)], slab.at[slot], wsem.at[slot])

    def tail_slot(chunk):
        return ((GROUPS - RING // 3 + chunk // 3) % (RING // 3)) * 3 + chunk % 3

    def tail_load(chunk):
        return pltpu.make_async_copy(wo_flat.at[pl.ds(2048, 2048), pl.ds(chunk * GROUP, GROUP)],
                                     slab.at[tail_slot(chunk)], wsem.at[tail_slot(chunk)])

    def head_load(tile):
        return pltpu.make_async_copy(wo.at[0, :, :, :, :, :, columns(tile)], p1.at[tile], hsem.at[tile])

    def for_tiles(body):
        short = min(bounds[c + 1] - bounds[c] for c in range(3))

        @pl.loop(0, short)
        def _(step):
            for c in range(3):
                body(c, bounds[c] + step)
        for c in range(3):
            for tile in range(bounds[c] + short, bounds[c + 1]):
                body(c, tile)

    def start_first(c, tile):
        for hop in range(1, 4):
            first_copy(c, tile, hop).start()
        own_copy(c, tile).start()

    for_tiles(start_first)

    qkv[1] = jnp.zeros(qkv.shape[1:], jnp.bfloat16)
    keys_t[1] = jnp.zeros(keys_t.shape[1:], jnp.bfloat16)

    for dim in range(3):
        for i, (src, dst) in enumerate(routing):
            pltpu.make_async_copy(src, dst.at[dim, 0], ms.at[i, dim, 0]).wait()
        for hop in range(1, 4):
            for copy in meta_copies(dim, hop):
                copy.wait_recv()
    lane = lax.broadcasted_iota(jnp.int32, (1, 128), 1)
    for c in range(3):
        d1, d2, d3 = c, (c + 1) % 3, (c + 2) % 3
        hop1 = (lane // 32) % 4
        local = lane % 32
        first = ((coords[d1] - hop1 + 4) % 4) * STRIDES[d1] + coords[d3] * STRIDES[d3]

        @pl.loop(0, 4)
        def _(w):
            owner = coords[d1] * STRIDES[d1] + coords[d2] * STRIDES[d2] + lax.rem(coords[d3] + w, 4) * STRIDES[d3]
            slot = slots_all[d3, w]
            flat = jnp.where(slot >= 0, ids_all[d3, w] * 16 + slot - owner * 16, -1)
            table = jnp.transpose(jnp.concatenate([flat.astype(jnp.float32), gates_all[d3, w]], axis=0))
            for hop2 in range(4):
                src = first + lax.rem(coords[d2] - hop2 + 4, 4) * STRIDES[d2]
                row_id = (src * 32 + local).astype(jnp.float32)
                gate = jnp.zeros((128, 128), jnp.float32)
                for j in range(8):
                    gate = jnp.where(table[:, j:j + 1] == row_id, table[:, 8 + j:9 + j], gate)
                high = jnp.minimum(gate, BF16_MAX).astype(jnp.bfloat16)
                rest = gate - high.astype(jnp.float32)
                mid = rest.astype(jnp.bfloat16)
                low = (rest - mid.astype(jnp.float32)).astype(jnp.bfloat16)
                gates[c, w, 0:128, hop2 * 128:hop2 * 128 + 128] = high
                gates[c, w, 128:256, hop2 * 128:hop2 * 128 + 128] = mid
                gates[c, w, 256:384, hop2 * 128:hop2 * 128 + 128] = low

    def relay(c, tile):
        own_copy(c, tile).wait()
        for hop in range(1, 4):
            first_copy(c, tile, hop).wait_recv()
        for hop in range(1, 4):
            second_copy(c, tile, hop).start()

    for_tiles(relay)

    for group in range(RING // 3):
        for i in range(3):
            qkv_load(group, i).start()

    def partial_sums(c, tile):
        dim2, dim3 = (c + 1) % 3, (c + 2) % 3
        for hop in range(1, 4):
            second_copy(c, tile, hop).wait_recv()

        @pl.loop(0, 4)
        def _(w):
            coord = lax.rem(coords[dim3] + w, 4)
            own = coords[dim2]
            if c == 1:
                blocks = [p1[tile, :, :, own, coord]]
            else:
                blocks = [p1[tile, :, :, coord, own]]
            blocks += [p2[tile, hop, :, :, coord] for hop in range(3)]
            rows = jnp.concatenate([b.reshape(128, 128) for b in blocks], axis=0)
            parts = jnp.dot(gates[c, w], rows, preferred_element_type=jnp.float32)
            s3[tile, w] = parts[0:128] + parts[128:256] + parts[256:384]
            third_copy(c, tile, w).start()

    for_tiles(partial_sums)

    def reuse(c, tile):
        for hop in range(1, 4):
            second_copy(c, tile, hop).wait_send()
        head_load(tile).start()

    for_tiles(reuse)

    resid_copy.wait_recv()

    @pl.loop(0, 4)
    def _(part):
        cols = pl.ds(pl.multiple_of(part * 512, 512), 512)

        @pl.loop(0, 4)
        def _(quarter):
            for hop in range(4):
                third_wait(part * 4 + quarter, hop)
        total = res_buf[:, cols].astype(jnp.float32)
        for hop in range(4):
            total = total + r3[hop, :, cols]
        y_ref[:, cols] = total.astype(jnp.bfloat16)

    y_float = y_ref[...].astype(jnp.float32)
    scale = lax.rsqrt(jnp.sum(y_float * y_float, axis=-1, keepdims=True) * (1.0 / y_ref.shape[1]) + NORM_EPS)
    x_ref[...] = (y_float * scale * gain[...]).astype(jnp.bfloat16)

    rows = lax.broadcasted_iota(jnp.int32, (128, 128), 0)
    keys = lax.broadcasted_iota(jnp.int32, (128, 128), 1)
    causal = rows >= keys

    def attend(group, half):
        outs = []
        for head in range(GROUP // 128):
            lanes = slice(head * 128, head * 128 + 128)
            score = jnp.dot(qkv[half, 0, :, lanes], keys_t[half, lanes, :], preferred_element_type=jnp.float32)
            score = jnp.where(causal, score * 128 ** -0.5, -jnp.inf)
            weight = jnp.exp(score - jnp.max(score, axis=-1, keepdims=True))
            prob = (weight * (1.0 / jnp.sum(weight, axis=-1, keepdims=True))).astype(jnp.bfloat16)
            outs.append(jnp.dot(prob, qkv[half, 1, :, lanes], preferred_element_type=jnp.float32).astype(jnp.bfloat16))
        context[:, pl.ds(pl.multiple_of(group * GROUP, GROUP), GROUP)] = jnp.concatenate(outs, axis=1)

    @pl.loop(0, GROUPS)
    def _(group):
        base = lax.rem(group, RING // 3) * 3
        half = lax.rem(group, 2)
        for i in range(3):
            slab_wait(base + i)
        attend(jnp.maximum(group - 1, 0), 1 - half)
        for i in range(3):
            part = jnp.dot(x_ref[...], slab[base + i], preferred_element_type=jnp.float32).astype(jnp.bfloat16)
            if i == 1:
                keys_t[half] = jnp.transpose(part)
            else:
                qkv[half, i // 2] = part

        @pl.when(group + RING // 3 < GROUPS)
        def _():
            for i in range(3):
                qkv_load(group + RING // 3, i).start()
        for late in range(CHUNKS):
            @pl.when(group == GROUPS - RING // 3 + late // 3)
            def _():
                tail_load(late).start()

    for piece in range(CHUNKS):
        tail_load(piece).wait()
        for i in range(GROUP // 128):
            head_load(piece * (GROUP // 128) + i).wait()
    attend(GROUPS - 1, (GROUPS - 1) % 2)
    early = [jnp.dot(context[:, 0:2048], jnp.concatenate([p1[chunk * 4 + i].reshape(2048, 128) for i in range(4)], axis=1),
                     preferred_element_type=jnp.float32) for chunk in range(CHUNKS)]
    for chunk in range(CHUNKS):
        total = early[chunk] + jnp.dot(context[:, 2048:4096], slab[tail_slot(chunk)], preferred_element_type=jnp.float32)
        cols = slice(chunk * GROUP, chunk * GROUP + GROUP)
        out_ref[:, cols] = (y_ref[:, cols].astype(jnp.float32) + total.astype(jnp.bfloat16).astype(jnp.float32)).astype(jnp.bfloat16)

    def drain(c, tile):
        for hop in range(1, 4):
            first_copy(c, tile, hop).wait_send()
        for hop in range(4):
            third_copy(c, tile, hop).wait_send()

    for_tiles(drain)
    for dim in range(3):
        for hop in range(1, 4):
            for copy in meta_copies(dim, hop):
                copy.wait_send()
    resid_copy.wait_send()


def run_stage(eo, ids, slots, gate_in, resid, gain, wq, wk, wv, wo):
    tiles = eo.shape[-1] // 128
    bounds = (0, tiles // 3, 2 * (tiles // 3), tiles)
    dma = pltpu.SemaphoreType.DMA
    hbm = pl.BlockSpec(memory_space=pl.ANY)
    vmem = pl.BlockSpec(memory_space=pltpu.VMEM)
    return pl.pallas_call(
        functools.partial(stage_kernel, bounds),
        out_shape=jax.ShapeDtypeStruct(resid.shape, jnp.bfloat16),
        in_specs=[hbm, hbm, hbm, hbm, hbm, vmem, hbm, hbm, hbm, hbm, hbm],
        out_specs=vmem,
        scratch_shapes=[
            pltpu.VMEM((tiles, 4, 2, 4, 4, 16, 128), jnp.bfloat16),
            pltpu.VMEM((tiles, 3, 4, 2, 4, 16, 128), jnp.bfloat16),
            pltpu.VMEM((tiles, 4, 128, 128), jnp.float32),
            pltpu.VMEM((4, 128, tiles * 128), jnp.float32),
            pltpu.VMEM((3, 4, 8, 128), jnp.int32),
            pltpu.VMEM((3, 4, 8, 128), jnp.int32),
            pltpu.VMEM((3, 4, 8, 128), jnp.float32),
            pltpu.VMEM((3, 4, 384, 512), jnp.bfloat16),
            pltpu.VMEM(resid.shape, jnp.bfloat16),
            pltpu.VMEM(resid.shape, jnp.bfloat16),
            pltpu.VMEM(resid.shape, jnp.bfloat16),
            pltpu.VMEM((2, 2, 128, GROUP), jnp.bfloat16),
            pltpu.VMEM((128, wq.shape[1]), jnp.bfloat16),
            pltpu.VMEM((RING, 2048, GROUP), jnp.bfloat16),
            dma((tiles, 4)), dma((tiles, 4)), dma((tiles, 3)), dma((tiles, 3)), dma((tiles, 4)), dma((tiles, 4)),
            dma((3, 3, 4)), dma((3, 3, 4)), dma, dma, dma((RING,)), dma((tiles,)), pltpu.VMEM((2, GROUP, 128), jnp.bfloat16),
        ],
        compiler_params=pltpu.CompilerParams(collective_id=0, has_side_effects=True, vmem_limit_bytes=67043328),
    )(eo, ids, slots, gate_in, resid, gain, wq, wk, wv, wo.reshape(2, 4, 2, 4, 4, 16, wo.shape[1]), wo)


def solution(mesh):
    token_spec = P(('data', 'pp'), None, 'ep', None, None)
    weight_spec = P('pp', None, None)

    def local_step(expert_out, expert_ids, slot_ids, gates, resid, norm_scale, w_query, w_key, w_value, w_out):
        eo = expert_out.reshape(2, 4, 4, 4, 16, expert_out.shape[-1])
        result = run_stage(eo, expert_ids[0, 0, 0].T, slot_ids[0, 0, 0].T, gates[0, 0, 0].T, resid[0, 0, 0], norm_scale,
                           w_query[0], w_key[0], w_value[0], w_out[0].reshape(-1, w_out.shape[-1]))
        return result[None, None, None]

    return jax.shard_map(local_step, mesh=mesh, in_specs=(token_spec, token_spec, token_spec, token_spec, token_spec, P('pp', None), weight_spec, weight_spec, weight_spec, P('pp', None, None, None)), out_specs=token_spec, check_vma=False)
```

```python
import functools
import jax
import jax.numpy as jnp
from jax import lax
from jax.experimental import pallas as pl
from jax.experimental.pallas import tpu as pltpu
from jax.sharding import PartitionSpec as P

NORM_EPS = 1e-6
MESH = pl.DeviceIdType.MESH
STRIDES = (1, 4, 16)
BF16_MAX = 3.3895313892515355e38
GROUP = 512
GROUPS = 8
CHUNKS = 4
RING = 12
LAST = (GROUPS - RING // 3) % (RING // 3) * 3


def axis_coord(me, dim):
    return lax.rem(lax.div(me, STRIDES[dim]), 4)


def mate_of(me, dim, hop):
    coord = axis_coord(me, dim)
    return me + (lax.rem(coord + hop, 4) - coord) * STRIDES[dim]


def stage_kernel(bounds, eo, ids, slots, gate_in, resid, gain_in, wq, wk, wv, wo_first, wo_second, wo, out_ref, p1, p2, s3, r3, ids_all, slots_all,
                 gates_all, gates, res_buf, y_ref, x_ref, query, context, slab, p1s, p1r, p2s, p2r, p3s, p3r, ms, mr, rs, rr, wsem, hsem, lsem, keys_t, values,
                 square_sum, out_buf, osem, gain, gsem):
    me = lax.axis_index('ep')
    pp = lax.axis_index('pp')
    other = 1 - pp
    coords = tuple(axis_coord(me, dim) for dim in range(3))

    barrier = pltpu.get_barrier_semaphore()
    for dim in range(3):
        for hop in range(1, 4):
            for stage in (pp, other):
                pl.semaphore_signal(barrier, inc=1, device_id={'pp': stage, 'ep': mate_of(me, dim, hop)}, device_id_type=MESH)
    pl.semaphore_signal(barrier, inc=1, device_id={'pp': other, 'ep': me}, device_id_type=MESH)
    pl.semaphore_wait(barrier, 19)

    routing = ((ids, ids_all), (slots, slots_all), (gate_in, gates_all))

    def meta_copies(dim, hop):
        return [pltpu.make_async_remote_copy(src, dst.at[dim, hop], ms.at[i, dim, hop], mr.at[i, dim, hop],
                                             device_id={'pp': pp, 'ep': mate_of(me, dim, 4 - hop)}, device_id_type=MESH)
                for i, (src, dst) in enumerate(routing)]

    for dim in range(3):
        for hop in range(1, 4):
            for copy in meta_copies(dim, hop):
                copy.start()
    for dim in range(3):
        for i, (src, dst) in enumerate(routing):
            pltpu.make_async_copy(src, dst.at[dim, 0], ms.at[i, dim, 0]).start()
    resid_copy = pltpu.make_async_remote_copy(resid, res_buf, rs, rr, device_id={'pp': other, 'ep': me}, device_id_type=MESH)
    resid_copy.start()
    gain_copy = pltpu.make_async_copy(gain_in, gain, gsem)
    gain_copy.start()

    def columns(tile):
        return pl.ds(pl.multiple_of(tile * 128, 128), 128)

    def rows_for(dim, coord, tile):
        if dim == 0:
            return eo.at[:, :, :, coord, :, columns(tile)]
        if dim == 1:
            return eo.at[:, :, coord, :, :, columns(tile)]
        return eo.at[:, coord, :, :, :, columns(tile)]

    def first_copy(c, tile, hop):
        return pltpu.make_async_remote_copy(rows_for(c, lax.rem(coords[c] + hop, 4), tile), p1.at[tile, hop],
                                            p1s.at[tile, hop], p1r.at[tile, hop],
                                            device_id={'pp': pp, 'ep': mate_of(me, c, hop)}, device_id_type=MESH)

    def own_copy(c, tile):
        return pltpu.make_async_copy(rows_for(c, coords[c], tile), p1.at[tile, 0], p1r.at[tile, 0])

    def second_copy(c, tile, hop):
        dim = (c + 1) % 3
        coord = lax.rem(coords[dim] + hop, 4)
        src = p1.at[tile, :, :, coord] if c == 1 else p1.at[tile, :, :, :, coord]
        return pltpu.make_async_remote_copy(src, p2.at[tile, hop - 1], p2s.at[tile, hop - 1], p2r.at[tile, hop - 1],
                                            device_id={'pp': pp, 'ep': mate_of(me, dim, hop)}, device_id_type=MESH)

    def third_copy(c, tile, hop):
        dim = (c + 2) % 3
        return pltpu.make_async_remote_copy(s3.at[tile, hop], r3.at[hop, :, columns(tile)], p3s.at[tile, hop], p3r.at[tile, hop],
                                            device_id={'pp': other, 'ep': mate_of(me, dim, hop)}, device_id_type=MESH)

    def slab_wait(slot):
        pltpu.make_async_copy(wq.at[:, pl.ds(0, GROUP)], slab.at[slot], wsem.at[slot]).wait()

    def qkv_load(group, i):
        slot = lax.rem(group, RING // 3) * 3 + i
        return pltpu.make_async_copy((wq, wk, wv)[i].at[:, pl.ds(pl.multiple_of(group * GROUP, GROUP), GROUP)], slab.at[slot], wsem.at[slot])

    def tail_load(chunk):
        return pltpu.make_async_copy(wo.at[pl.ds(3584, 512), pl.ds(chunk * GROUP, GROUP)], slab.at[LAST, pl.ds(chunk * 512, 512)], lsem.at[chunk])

    def store_copy(chunk):
        return pltpu.make_async_copy(out_buf.at[chunk], out_ref.at[:, pl.ds(chunk * GROUP, GROUP)], osem.at[chunk])

    def head_load(tile):
        return pltpu.make_async_copy(wo_first.at[pl.ds(0, 4), :, :, :, :, columns(tile)], p1.at[tile], hsem.at[0, tile])

    def middle_load(tile):
        return pltpu.make_async_copy(wo_second.at[pl.ds(4, 3), :, :, :, :, columns(tile)], p2.at[tile], hsem.at[1, tile])

    def for_tiles(body):
        short = min(bounds[c + 1] - bounds[c] for c in range(3))

        @pl.loop(0, short)
        def _(step):
            for c in range(3):
                body(c, bounds[c] + step)
        for c in range(3):
            for tile in range(bounds[c] + short, bounds[c + 1]):
                body(c, tile)

    def start_first(c, tile):
        for hop in range(1, 4):
            first_copy(c, tile, hop).start()
        own_copy(c, tile).start()

    for_tiles(start_first)

    query[1] = jnp.zeros(query.shape[1:], jnp.bfloat16)
    keys_t[...] = jnp.zeros(keys_t.shape, jnp.bfloat16)
    values[...] = jnp.zeros(values.shape, jnp.bfloat16)

    for dim in range(3):
        for i, (src, dst) in enumerate(routing):
            pltpu.make_async_copy(src, dst.at[dim, 0], ms.at[i, dim, 0]).wait()
        for hop in range(1, 4):
            for copy in meta_copies(dim, hop):
                copy.wait_recv()
    lane = lax.broadcasted_iota(jnp.int32, (1, 128), 1)
    for c in range(3):
        d1, d2, d3 = c, (c + 1) % 3, (c + 2) % 3
        hop1 = (lane // 32) % 4
        local = lane % 32
        first = ((coords[d1] - hop1 + 4) % 4) * STRIDES[d1] + coords[d3] * STRIDES[d3]

        @pl.loop(0, 4)
        def _(w):
            owner = coords[d1] * STRIDES[d1] + coords[d2] * STRIDES[d2] + lax.rem(coords[d3] + w, 4) * STRIDES[d3]
            slot = slots_all[d3, w]
            flat = jnp.where(slot >= 0, ids_all[d3, w] * 16 + slot - owner * 16, -1)
            table = jnp.transpose(jnp.concatenate([flat.astype(jnp.float32), gates_all[d3, w]], axis=0))
            for hop2 in range(4):
                src = first + lax.rem(coords[d2] - hop2 + 4, 4) * STRIDES[d2]
                row_id = (src * 32 + local).astype(jnp.float32)
                gate = jnp.zeros((128, 128), jnp.float32)
                for j in range(8):
                    gate = jnp.where(table[:, j:j + 1] == row_id, table[:, 8 + j:9 + j], gate)
                high = jnp.minimum(gate, BF16_MAX).astype(jnp.bfloat16)
                rest = gate - high.astype(jnp.float32)
                mid = rest.astype(jnp.bfloat16)
                low = (rest - mid.astype(jnp.float32)).astype(jnp.bfloat16)
                gates[c, w, 0:128, hop2 * 128:hop2 * 128 + 128] = high
                gates[c, w, 128:256, hop2 * 128:hop2 * 128 + 128] = mid
                gates[c, w, 256:384, hop2 * 128:hop2 * 128 + 128] = low

    def relay(c, tile):
        own_copy(c, tile).wait()
        for hop in range(1, 4):
            first_copy(c, tile, hop).wait_recv()
        for hop in range(1, 4):
            second_copy(c, tile, hop).start()

    for_tiles(relay)

    for group in range(RING // 3):
        for i in range(3):
            qkv_load(group, i).start()

    def partial_sums(c, tile):
        dim2, dim3 = (c + 1) % 3, (c + 2) % 3
        for hop in range(1, 4):
            second_copy(c, tile, hop).wait_recv()

        @pl.loop(0, 4)
        def _(step):
            w = lax.rem(step + 2, 4)
            coord = lax.rem(coords[dim3] + w, 4)
            own = coords[dim2]
            if c == 1:
                blocks = [p1[tile, :, :, own, coord]]
            else:
                blocks = [p1[tile, :, :, coord, own]]
            blocks += [p2[tile, hop, :, :, coord] for hop in range(3)]
            rows = jnp.concatenate([b.reshape(128, 128) for b in blocks], axis=0)
            parts = jnp.dot(gates[c, w], rows, preferred_element_type=jnp.float32)
            s3[tile, w] = parts[0:128] + parts[128:256] + parts[256:384]
        for hop in range(4):
            third_copy(c, tile, hop).start()

    for_tiles(partial_sums)

    def reuse(c, tile):
        for hop in range(1, 4):
            first_copy(c, tile, hop).wait_send()
            second_copy(c, tile, hop).wait_send()
        head_load(tile).start()
        middle_load(tile).start()

    for_tiles(reuse)

    resid_copy.wait_recv()
    gain_copy.wait()

    for dim in range(3):
        for hop in range(1, 4):
            for copy in meta_copies(dim, hop):
                copy.wait_send()
    resid_copy.wait_send()
    square_sum[...] = jnp.zeros(square_sum.shape, jnp.float32)

    def finish(c, tile):
        for hop in range(4):
            third_copy(c, tile, hop).wait_recv()
        cols = columns(tile)
        total = res_buf[:, cols].astype(jnp.float32)
        for i in range(4):
            total = total + r3[i, :, cols]
        rounded = total.astype(jnp.bfloat16)
        y_ref[:, cols] = rounded
        square_sum[...] += rounded.astype(jnp.float32) * rounded.astype(jnp.float32)

    for_tiles(finish)

    scale = lax.rsqrt(jnp.sum(square_sum[...], axis=-1, keepdims=True) * (1.0 / y_ref.shape[1]) + NORM_EPS)

    @pl.loop(0, 4)
    def _(part):
        cols = pl.ds(pl.multiple_of(part * GROUP, GROUP), GROUP)
        x_ref[:, cols] = (y_ref[:, cols].astype(jnp.float32) * scale * gain[:, cols]).astype(jnp.bfloat16)

    rows = lax.broadcasted_iota(jnp.int32, (128, 128), 0)
    keys = lax.broadcasted_iota(jnp.int32, (128, 128), 1)
    causal = rows >= keys

    def attend_pair(group, half, pair):
        lanes = slice(pair * 256, pair * 256 + 256)
        scores = jnp.dot(query[half, :, lanes], keys_t[half, pair], preferred_element_type=jnp.float32)
        probs = []
        for head in range(2):
            score = jnp.where(causal, scores[:, head * 128:head * 128 + 128] * 128 ** -0.5, -jnp.inf)
            weight = jnp.exp(score - jnp.max(score, axis=-1, keepdims=True))
            probs.append((weight * (1.0 / jnp.sum(weight, axis=-1, keepdims=True))).astype(jnp.bfloat16))
        mixed = jnp.dot(jnp.concatenate(probs, axis=1), values[half, pair], preferred_element_type=jnp.float32).astype(jnp.bfloat16)
        context[:, pl.ds(pl.multiple_of(group * GROUP + pair * 256, 256), 256)] = mixed

    def project(base, half, i):
        part = jnp.dot(x_ref[...], slab[base + i], preferred_element_type=jnp.float32).astype(jnp.bfloat16)
        if i == 0:
            query[half] = part
            return
        if i == 1:
            part = jnp.transpose(part)
        for head in range(GROUP // 128):
            block = slice(head % 2 * 128, head % 2 * 128 + 128)
            if i == 1:
                keys_t[half, head // 2, block, block] = part[head * 128:head * 128 + 128, :]
            else:
                values[half, head // 2, block, block] = part[:, head * 128:head * 128 + 128]

    def group_step(group, half):
        base = lax.rem(group, RING // 3) * 3
        for i in range(3):
            slab_wait(base + i)
        before = jnp.maximum(group - 1, 0)
        for i in range(3):
            project(base, half, i)
        for pair in range(2):
            attend_pair(before, 1 - half, pair)

        @pl.when(group + RING // 3 < GROUPS)
        def _():
            for i in range(3):
                qkv_load(group + RING // 3, i).start()
        @pl.when(group == GROUPS - RING // 3)
        def _():
            for chunk in range(CHUNKS):
                tail_load(chunk).start()

    @pl.loop(0, GROUPS // 2)
    def _(pair):
        for half in range(2):
            group_step(pair * 2 + half, half)

    for piece in range(CHUNKS):
        tail_load(piece).wait()
        for i in range(GROUP // 128):
            head_load(piece * (GROUP // 128) + i).wait()
            middle_load(piece * (GROUP // 128) + i).wait()
    for pair in range(2):
        attend_pair(GROUPS - 1, (GROUPS - 1) % 2, pair)

    early = [jnp.dot(context[:, 0:2048], jnp.concatenate([p1[chunk * 4 + i].reshape(2048, 128) for i in range(4)], axis=1),
                     preferred_element_type=jnp.float32) for chunk in range(CHUNKS)]
    for chunk in range(CHUNKS):
        middle = jnp.concatenate([p2[chunk * 4 + i].reshape(1536, 128) for i in range(4)], axis=1)
        total = early[chunk] + jnp.dot(context[:, 2048:3584], middle, preferred_element_type=jnp.float32)
        total = total + jnp.dot(context[:, 3584:4096], slab[LAST, chunk * 512:chunk * 512 + 512], preferred_element_type=jnp.float32)
        cols = slice(chunk * GROUP, chunk * GROUP + GROUP)
        out_buf[chunk] = (y_ref[:, cols].astype(jnp.float32) + total.astype(jnp.bfloat16).astype(jnp.float32)).astype(jnp.bfloat16)
        store_copy(chunk).start()

    def settle(c, tile):
        for hop in range(4):
            third_copy(c, tile, hop).wait_send()


    for_tiles(settle)

    for chunk in range(CHUNKS):
        store_copy(chunk).wait()


def run_stage(eo, ids, slots, gate_in, resid, gain, wq, wk, wv, wo):
    tiles = eo.shape[-1] // 128
    bounds = (0, tiles // 3, 2 * (tiles // 3), tiles)
    dma = pltpu.SemaphoreType.DMA
    hbm = pl.BlockSpec(memory_space=pl.ANY)
    return pl.pallas_call(
        functools.partial(stage_kernel, bounds),
        out_shape=jax.ShapeDtypeStruct(resid.shape, jnp.bfloat16),
        in_specs=[hbm] * 12,
        out_specs=hbm,
        scratch_shapes=[
            pltpu.VMEM((tiles, 4, 2, 4, 4, 16, 128), jnp.bfloat16),
            pltpu.VMEM((tiles, 3, 4, 2, 4, 16, 128), jnp.bfloat16),
            pltpu.VMEM((tiles, 4, 128, 128), jnp.float32),
            pltpu.VMEM((4, 128, tiles * 128), jnp.float32),
            pltpu.VMEM((3, 4, 8, 128), jnp.int32),
            pltpu.VMEM((3, 4, 8, 128), jnp.int32),
            pltpu.VMEM((3, 4, 8, 128), jnp.float32),
            pltpu.VMEM((3, 4, 384, 512), jnp.bfloat16),
            pltpu.VMEM(resid.shape, jnp.bfloat16),
            pltpu.VMEM(resid.shape, jnp.bfloat16),
            pltpu.VMEM(resid.shape, jnp.bfloat16),
            pltpu.VMEM((2, 128, GROUP), jnp.bfloat16),
            pltpu.VMEM((128, wq.shape[1]), jnp.bfloat16),
            pltpu.VMEM((RING, 2048, GROUP), jnp.bfloat16),
            dma((tiles, 4)), dma((tiles, 4)), dma((tiles, 3)), dma((tiles, 3)), dma((tiles, 4)), dma((tiles, 4)),
            dma((3, 3, 4)), dma((3, 3, 4)), dma, dma, dma((RING,)), dma((2, tiles)), dma((CHUNKS,)), pltpu.VMEM((2, 2, 256, 256), jnp.bfloat16), pltpu.VMEM((2, 2, 256, 256), jnp.bfloat16),
            pltpu.VMEM((128, 128), jnp.float32),
            pltpu.VMEM((CHUNKS, 128, GROUP), jnp.bfloat16), dma((CHUNKS,)), pltpu.VMEM((1, resid.shape[1]), jnp.float32), dma,
        ],
        compiler_params=pltpu.CompilerParams(collective_id=0, has_side_effects=True, vmem_limit_bytes=67043328),
    )(eo, ids, slots, gate_in, resid, gain, wq, wk, wv, wo.reshape(8, 2, 4, 4, 16, wo.shape[1]), wo.reshape(8, 4, 2, 4, 16, wo.shape[1]), wo)


def solution(mesh):
    token_spec = P(('data', 'pp'), None, 'ep', None, None)
    weight_spec = P('pp', None, None)

    def local_step(expert_out, expert_ids, slot_ids, gates, resid, norm_scale, w_query, w_key, w_value, w_out):
        eo = expert_out.reshape(2, 4, 4, 4, 16, expert_out.shape[-1])
        result = run_stage(eo, expert_ids[0, 0, 0].T, slot_ids[0, 0, 0].T, gates[0, 0, 0].T, resid[0, 0, 0], norm_scale,
                           w_query[0], w_key[0], w_value[0], w_out[0].reshape(-1, w_out.shape[-1]))
        return result[None, None, None]

    return jax.shard_map(local_step, mesh=mesh, in_specs=(token_spec, token_spec, token_spec, token_spec, token_spec, P('pp', None), weight_spec, weight_spec, weight_spec, P('pp', None, None, None)), out_specs=token_spec, check_vma=False)
```

```python
import functools
import jax
import jax.numpy as jnp
from jax import lax
from jax.experimental import pallas as pl
from jax.experimental.pallas import tpu as pltpu
from jax.sharding import PartitionSpec as P

NORM_EPS = 1e-6
MESH = pl.DeviceIdType.MESH
STRIDES = (1, 4, 16)
BF16_MAX = 3.3895313892515355e38
GROUP = 512
GROUPS = 8
CHUNKS = 4
RING = 12
LAST = (GROUPS - RING // 3) % (RING // 3) * 3


def axis_coord(me, dim):
    return lax.rem(lax.div(me, STRIDES[dim]), 4)


def mate_of(me, dim, hop):
    coord = axis_coord(me, dim)
    return me + (lax.rem(coord + hop, 4) - coord) * STRIDES[dim]


def stage_kernel(bounds, eo, ids, slots, gate_in, resid, gain_in, wq, wk, wv, wo_first, wo_second, wo, out_ref, p1, p2, s3, r3, ids_all, slots_all,
                 gates_all, gates, res_buf, y_ref, x_ref, query, context, slab, p1s, p1r, p2s, p2r, p3s, p3r, ms, mr, rs, rr, wsem, hsem, lsem, keys_t, values,
                 square_sum, out_buf, osem, gain, gsem):
    me = lax.axis_index('ep')
    pp = lax.axis_index('pp')
    other = 1 - pp
    coords = tuple(axis_coord(me, dim) for dim in range(3))

    barrier = pltpu.get_barrier_semaphore()
    for dim in range(3):
        for hop in range(1, 4):
            for stage in (pp, other):
                pl.semaphore_signal(barrier, inc=1, device_id={'pp': stage, 'ep': mate_of(me, dim, hop)}, device_id_type=MESH)
    pl.semaphore_signal(barrier, inc=1, device_id={'pp': other, 'ep': me}, device_id_type=MESH)
    pl.semaphore_wait(barrier, 19)

    routing = ((ids, ids_all), (slots, slots_all), (gate_in, gates_all))

    def meta_copies(dim, hop):
        return [pltpu.make_async_remote_copy(src, dst.at[dim, hop], ms.at[i, dim, hop], mr.at[i, dim, hop],
                                             device_id={'pp': pp, 'ep': mate_of(me, dim, 4 - hop)}, device_id_type=MESH)
                for i, (src, dst) in enumerate(routing)]

    def columns(tile):
        return pl.ds(pl.multiple_of(tile * 128, 128), 128)

    def rows_for(dim, coord, tile):
        if dim == 0:
            return eo.at[:, :, :, coord, :, columns(tile)]
        if dim == 1:
            return eo.at[:, :, coord, :, :, columns(tile)]
        return eo.at[:, coord, :, :, :, columns(tile)]

    def first_copy(c, tile, hop):
        return pltpu.make_async_remote_copy(rows_for(c, lax.rem(coords[c] + hop, 4), tile), p1.at[tile, hop],
                                            p1s.at[tile, hop], p1r.at[tile, hop],
                                            device_id={'pp': pp, 'ep': mate_of(me, c, hop)}, device_id_type=MESH)

    def own_copy(c, tile):
        return pltpu.make_async_copy(rows_for(c, coords[c], tile), p1.at[tile, 0], p1r.at[tile, 0])

    def second_copy(c, tile, hop):
        dim = (c + 1) % 3
        coord = lax.rem(coords[dim] + hop, 4)
        src = p1.at[tile, :, :, coord] if c == 1 else p1.at[tile, :, :, :, coord]
        return pltpu.make_async_remote_copy(src, p2.at[tile, hop - 1], p2s.at[tile, hop - 1], p2r.at[tile, hop - 1],
                                            device_id={'pp': pp, 'ep': mate_of(me, dim, hop)}, device_id_type=MESH)

    def third_copy(c, tile, hop):
        dim = (c + 2) % 3
        return pltpu.make_async_remote_copy(s3.at[tile, hop], r3.at[hop, :, columns(tile)], p3s.at[tile, hop], p3r.at[tile, hop],
                                            device_id={'pp': other, 'ep': mate_of(me, dim, hop)}, device_id_type=MESH)

    def slab_wait(slot):
        pltpu.make_async_copy(wq.at[:, pl.ds(0, GROUP)], slab.at[slot], wsem.at[slot]).wait()

    def qkv_load(group, i):
        slot = lax.rem(group, RING // 3) * 3 + i
        return pltpu.make_async_copy((wq, wk, wv)[i].at[:, pl.ds(pl.multiple_of(group * GROUP, GROUP), GROUP)], slab.at[slot], wsem.at[slot])

    def tail_load(chunk):
        return pltpu.make_async_copy(wo.at[pl.ds(3584, 512), pl.ds(chunk * GROUP, GROUP)], slab.at[LAST, pl.ds(chunk * 512, 512)], lsem.at[chunk])

    def store_copy(chunk):
        return pltpu.make_async_copy(out_buf.at[chunk], out_ref.at[:, pl.ds(chunk * GROUP, GROUP)], osem.at[chunk])

    def head_load(tile):
        return pltpu.make_async_copy(wo_first.at[pl.ds(0, 4), :, :, :, :, columns(tile)], p1.at[tile], hsem.at[0, tile])

    def middle_load(tile):
        return pltpu.make_async_copy(wo_second.at[pl.ds(4, 3), :, :, :, :, columns(tile)], p2.at[tile], hsem.at[1, tile])

    def for_tiles(body, start=0):
        short = min(bounds[c + 1] - bounds[c] for c in range(3))

        @pl.loop(start, short)
        def _(step):
            for c in range(3):
                body(c, bounds[c] + step)
        for c in range(3):
            for tile in range(bounds[c] + short, bounds[c + 1]):
                body(c, tile)

    def start_first(c, tile):
        for hop in range(1, 4):
            first_copy(c, tile, hop).start()
        own_copy(c, tile).start()

    for c in range(3):
        start_first(c, bounds[c])
    for dim in range(3):
        for hop in range(1, 4):
            for copy in meta_copies(dim, hop):
                copy.start()
    for dim in range(3):
        for i, (src, dst) in enumerate(routing):
            pltpu.make_async_copy(src, dst.at[dim, 0], ms.at[i, dim, 0]).start()
    resid_copy = pltpu.make_async_remote_copy(resid, res_buf, rs, rr, device_id={'pp': other, 'ep': me}, device_id_type=MESH)
    resid_copy.start()
    gain_copy = pltpu.make_async_copy(gain_in, gain, gsem)
    gain_copy.start()
    for_tiles(start_first, 1)

    query[1] = jnp.zeros(query.shape[1:], jnp.bfloat16)
    keys_t[...] = jnp.zeros(keys_t.shape, jnp.bfloat16)
    values[...] = jnp.zeros(values.shape, jnp.bfloat16)

    for dim in range(3):
        for i, (src, dst) in enumerate(routing):
            pltpu.make_async_copy(src, dst.at[dim, 0], ms.at[i, dim, 0]).wait()
        for hop in range(1, 4):
            for copy in meta_copies(dim, hop):
                copy.wait_recv()
    lane = lax.broadcasted_iota(jnp.int32, (1, 128), 1)
    for c in range(3):
        d1, d2, d3 = c, (c + 1) % 3, (c + 2) % 3
        hop1 = (lane // 32) % 4
        local = lane % 32
        first = ((coords[d1] - hop1 + 4) % 4) * STRIDES[d1] + coords[d3] * STRIDES[d3]

        @pl.loop(0, 4)
        def _(w):
            owner = coords[d1] * STRIDES[d1] + coords[d2] * STRIDES[d2] + lax.rem(coords[d3] + w, 4) * STRIDES[d3]
            slot = slots_all[d3, w]
            flat = jnp.where(slot >= 0, ids_all[d3, w] * 16 + slot - owner * 16, -1)
            table = jnp.transpose(jnp.concatenate([flat.astype(jnp.float32), gates_all[d3, w]], axis=0))
            for hop2 in range(4):
                src = first + lax.rem(coords[d2] - hop2 + 4, 4) * STRIDES[d2]
                row_id = (src * 32 + local).astype(jnp.float32)
                gate = jnp.zeros((128, 128), jnp.float32)
                for j in range(8):
                    gate = jnp.where(table[:, j:j + 1] == row_id, table[:, 8 + j:9 + j], gate)
                high = jnp.minimum(gate, BF16_MAX).astype(jnp.bfloat16)
                rest = gate - high.astype(jnp.float32)
                mid = rest.astype(jnp.bfloat16)
                low = (rest - mid.astype(jnp.float32)).astype(jnp.bfloat16)
                gates[c, w, 0:128, hop2 * 128:hop2 * 128 + 128] = high
                gates[c, w, 128:256, hop2 * 128:hop2 * 128 + 128] = mid
                gates[c, w, 256:384, hop2 * 128:hop2 * 128 + 128] = low

    def relay(c, tile):
        own_copy(c, tile).wait()
        for hop in range(1, 4):
            first_copy(c, tile, hop).wait_recv()
        for hop in range(1, 4):
            second_copy(c, tile, hop).start()

    for_tiles(relay)

    for group in range(RING // 3):
        for i in range(3):
            qkv_load(group, i).start()

    def partial_sums(c, tile):
        dim2, dim3 = (c + 1) % 3, (c + 2) % 3
        for hop in range(1, 4):
            second_copy(c, tile, hop).wait_recv()

        @pl.loop(0, 4)
        def _(step):
            w = lax.rem(step + 2, 4)
            coord = lax.rem(coords[dim3] + w, 4)
            own = coords[dim2]
            if c == 1:
                blocks = [p1[tile, :, :, own, coord]]
            else:
                blocks = [p1[tile, :, :, coord, own]]
            blocks += [p2[tile, hop, :, :, coord] for hop in range(3)]
            rows = jnp.concatenate([b.reshape(128, 128) for b in blocks], axis=0)
            parts = jnp.dot(gates[c, w], rows, preferred_element_type=jnp.float32)
            s3[tile, w] = parts[0:128] + parts[128:256] + parts[256:384]
        for hop in (2, 1, 3, 0):
            third_copy(c, tile, hop).start()

    for_tiles(partial_sums)

    def reuse(c, tile):
        for hop in range(1, 4):
            first_copy(c, tile, hop).wait_send()
            second_copy(c, tile, hop).wait_send()
        head_load(tile).start()
        middle_load(tile).start()

    for_tiles(reuse)

    resid_copy.wait_recv()
    gain_copy.wait()

    for dim in range(3):
        for hop in range(1, 4):
            for copy in meta_copies(dim, hop):
                copy.wait_send()
    resid_copy.wait_send()
    square_sum[...] = jnp.zeros(square_sum.shape, jnp.float32)

    def finish(c, tile):
        for hop in range(4):
            third_copy(c, tile, hop).wait_recv()
        cols = columns(tile)
        total = res_buf[:, cols].astype(jnp.float32)
        for i in range(4):
            total = total + r3[i, :, cols]
        rounded = total.astype(jnp.bfloat16)
        y_ref[:, cols] = rounded
        square_sum[...] += rounded.astype(jnp.float32) * rounded.astype(jnp.float32)

    for_tiles(finish)

    scale = lax.rsqrt(jnp.sum(square_sum[...], axis=-1, keepdims=True) * (1.0 / y_ref.shape[1]) + NORM_EPS)

    @pl.loop(0, 4)
    def _(part):
        cols = pl.ds(pl.multiple_of(part * GROUP, GROUP), GROUP)
        x_ref[:, cols] = (y_ref[:, cols].astype(jnp.float32) * scale * gain[:, cols]).astype(jnp.bfloat16)

    rows = lax.broadcasted_iota(jnp.int32, (128, 128), 0)
    keys = lax.broadcasted_iota(jnp.int32, (128, 128), 1)
    causal = rows >= keys

    def attend_pair(group, half, pair):
        lanes = slice(pair * 256, pair * 256 + 256)
        scores = jnp.dot(query[half, :, lanes], keys_t[half, pair], preferred_element_type=jnp.float32)
        probs = []
        for head in range(2):
            score = jnp.where(causal, scores[:, head * 128:head * 128 + 128] * 128 ** -0.5, -jnp.inf)
            weight = jnp.exp(score - jnp.max(score, axis=-1, keepdims=True))
            probs.append((weight * (1.0 / jnp.sum(weight, axis=-1, keepdims=True))).astype(jnp.bfloat16))
        mixed = jnp.dot(jnp.concatenate(probs, axis=1), values[half, pair], preferred_element_type=jnp.float32).astype(jnp.bfloat16)
        context[:, pl.ds(pl.multiple_of(group * GROUP + pair * 256, 256), 256)] = mixed

    def project(base, half, i):
        part = jnp.dot(x_ref[...], slab[base + i], preferred_element_type=jnp.float32).astype(jnp.bfloat16)
        if i == 0:
            query[half] = part
            return
        if i == 1:
            part = jnp.transpose(part)
        for head in range(GROUP // 128):
            block = slice(head % 2 * 128, head % 2 * 128 + 128)
            if i == 1:
                keys_t[half, head // 2, block, block] = part[head * 128:head * 128 + 128, :]
            else:
                values[half, head // 2, block, block] = part[:, head * 128:head * 128 + 128]

    def group_step(group, half):
        base = lax.rem(group, RING // 3) * 3
        for i in range(3):
            slab_wait(base + i)
        before = jnp.maximum(group - 1, 0)
        for i in range(3):
            project(base, half, i)
        for pair in range(2):
            attend_pair(before, 1 - half, pair)

        @pl.when(group + RING // 3 < GROUPS)
        def _():
            for i in range(3):
                qkv_load(group + RING // 3, i).start()
        @pl.when(group == GROUPS - RING // 3)
        def _():
            for chunk in range(CHUNKS):
                tail_load(chunk).start()

    @pl.loop(0, GROUPS // 2)
    def _(pair):
        for half in range(2):
            group_step(pair * 2 + half, half)

    for piece in range(CHUNKS):
        tail_load(piece).wait()
        for i in range(GROUP // 128):
            head_load(piece * (GROUP // 128) + i).wait()
            middle_load(piece * (GROUP // 128) + i).wait()
    for pair in range(2):
        attend_pair(GROUPS - 1, (GROUPS - 1) % 2, pair)

    early = [jnp.dot(context[:, 0:2048], jnp.concatenate([p1[chunk * 4 + i].reshape(2048, 128) for i in range(4)], axis=1),
                     preferred_element_type=jnp.float32) for chunk in range(CHUNKS)]
    for chunk in range(CHUNKS):
        middle = jnp.concatenate([p2[chunk * 4 + i].reshape(1536, 128) for i in range(4)], axis=1)
        total = early[chunk] + jnp.dot(context[:, 2048:3584], middle, preferred_element_type=jnp.float32)
        total = total + jnp.dot(context[:, 3584:4096], slab[LAST, chunk * 512:chunk * 512 + 512], preferred_element_type=jnp.float32)
        cols = slice(chunk * GROUP, chunk * GROUP + GROUP)
        out_buf[chunk] = (y_ref[:, cols].astype(jnp.float32) + total.astype(jnp.bfloat16).astype(jnp.float32)).astype(jnp.bfloat16)
        store_copy(chunk).start()

    def settle(c, tile):
        for hop in range(4):
            third_copy(c, tile, hop).wait_send()


    for_tiles(settle)

    for chunk in range(CHUNKS):
        store_copy(chunk).wait()


def run_stage(eo, ids, slots, gate_in, resid, gain, wq, wk, wv, wo):
    tiles = eo.shape[-1] // 128
    bounds = (0, tiles // 3, 2 * (tiles // 3), tiles)
    dma = pltpu.SemaphoreType.DMA
    hbm = pl.BlockSpec(memory_space=pl.ANY)
    return pl.pallas_call(
        functools.partial(stage_kernel, bounds),
        out_shape=jax.ShapeDtypeStruct(resid.shape, jnp.bfloat16),
        in_specs=[hbm] * 12,
        out_specs=hbm,
        scratch_shapes=[
            pltpu.VMEM((tiles, 4, 2, 4, 4, 16, 128), jnp.bfloat16),
            pltpu.VMEM((tiles, 3, 4, 2, 4, 16, 128), jnp.bfloat16),
            pltpu.VMEM((tiles, 4, 128, 128), jnp.float32),
            pltpu.VMEM((4, 128, tiles * 128), jnp.float32),
            pltpu.VMEM((3, 4, 8, 128), jnp.int32),
            pltpu.VMEM((3, 4, 8, 128), jnp.int32),
            pltpu.VMEM((3, 4, 8, 128), jnp.float32),
            pltpu.VMEM((3, 4, 384, 512), jnp.bfloat16),
            pltpu.VMEM(resid.shape, jnp.bfloat16),
            pltpu.VMEM(resid.shape, jnp.bfloat16),
            pltpu.VMEM(resid.shape, jnp.bfloat16),
            pltpu.VMEM((2, 128, GROUP), jnp.bfloat16),
            pltpu.VMEM((128, wq.shape[1]), jnp.bfloat16),
            pltpu.VMEM((RING, 2048, GROUP), jnp.bfloat16),
            dma((tiles, 4)), dma((tiles, 4)), dma((tiles, 3)), dma((tiles, 3)), dma((tiles, 4)), dma((tiles, 4)),
            dma((3, 3, 4)), dma((3, 3, 4)), dma, dma, dma((RING,)), dma((2, tiles)), dma((CHUNKS,)), pltpu.VMEM((2, 2, 256, 256), jnp.bfloat16), pltpu.VMEM((2, 2, 256, 256), jnp.bfloat16),
            pltpu.VMEM((128, 128), jnp.float32),
            pltpu.VMEM((CHUNKS, 128, GROUP), jnp.bfloat16), dma((CHUNKS,)), pltpu.VMEM((1, resid.shape[1]), jnp.float32), dma,
        ],
        compiler_params=pltpu.CompilerParams(collective_id=0, has_side_effects=True, vmem_limit_bytes=67043328),
    )(eo, ids, slots, gate_in, resid, gain, wq, wk, wv, wo.reshape(8, 2, 4, 4, 16, wo.shape[1]), wo.reshape(8, 4, 2, 4, 16, wo.shape[1]), wo)


def solution(mesh):
    token_spec = P(('data', 'pp'), None, 'ep', None, None)
    weight_spec = P('pp', None, None)

    def local_step(expert_out, expert_ids, slot_ids, gates, resid, norm_scale, w_query, w_key, w_value, w_out):
        eo = expert_out.reshape(2, 4, 4, 4, 16, expert_out.shape[-1])
        result = run_stage(eo, expert_ids[0, 0, 0].T, slot_ids[0, 0, 0].T, gates[0, 0, 0].T, resid[0, 0, 0], norm_scale,
                           w_query[0], w_key[0], w_value[0], w_out[0].reshape(-1, w_out.shape[-1]))
        return result[None, None, None]

    return jax.shard_map(local_step, mesh=mesh, in_specs=(token_spec, token_spec, token_spec, token_spec, token_spec, P('pp', None), weight_spec, weight_spec, weight_spec, P('pp', None, None, None)), out_specs=token_spec, check_vma=False)
```
